32 devices in a mesh: local: 4 (over z), data: 8 (over y, x, core).
Axes of the slice: x: 2, y: 2, z: 4, core: 2. Of those that a mesh axis runs over, the one named last changes fastest.
Arguments:
- tokens: bfloat16 [65536, 1024], P(('local', 'data'))
- grad_out: bfloat16 [65536, 1024], P(('local', 'data'))
- w_up: bfloat16 [2, 1024, 4096], P(None, ('local', 'data'))
- w_down: bfloat16 [2, 4096, 1024], P(None, ('local', 'data'))
Outputs:
- output 1: bfloat16 [65536, 1024], P(('local', 'data'))
- output 2: bfloat16 [65536, 1024], P(('local', 'data'))
- output 3: float32 [2, 1024, 4096], P(None, ('local', 'data'))
- output 4: float32 [2, 4096, 1024], P(None, ('local', 'data'))
All inputs are finite; a program needn't handle non-finite values.
Results may differ from the reference program's by a relative error of at most 0.0139185.
Values are sent between devices in bfloat16 or wider.
A program may use at most 1 GiB of HBM per device.

```python
import jax
import jax.numpy as jnp
from jax import lax

HIDDEN = 1024
FFN_DIM = 4096
NUM_LAYERS = 2
TOTAL_TOKENS = 65536
NORM_EPS = 1e-6
BLOCK_ROWS = min(TOTAL_TOKENS, 2048)


def setup_inputs(seed: int = 0) -> dict:
    keys = jax.random.split(jax.random.key(seed), 4)
    tokens = jax.random.normal(keys[0], (TOTAL_TOKENS, HIDDEN), jnp.float32).astype(jnp.bfloat16)
    grad_out = jax.random.normal(keys[1], (TOTAL_TOKENS, HIDDEN), jnp.float32).astype(jnp.bfloat16)
    w_up = (jax.random.normal(keys[2], (NUM_LAYERS, HIDDEN, FFN_DIM), jnp.float32) * HIDDEN ** -0.5).astype(jnp.bfloat16)
    w_down = (jax.random.normal(keys[3], (NUM_LAYERS, FFN_DIM, HIDDEN), jnp.float32) * (1.5 * FFN_DIM ** -0.5)).astype(jnp.bfloat16)
    return {'tokens': tokens, 'grad_out': grad_out, 'w_up': w_up, 'w_down': w_down}


def rms_norm(x_f32):
    return x_f32 * lax.rsqrt(jnp.mean(x_f32 * x_f32, axis=-1, keepdims=True) + NORM_EPS)


def gelu_tanh(values):
    return jax.nn.gelu(values, approximate=True)


def layer_forward(layer_in, up_w, down_w):
    x_f32 = layer_in.astype(jnp.float32)
    normed = rms_norm(x_f32).astype(jnp.bfloat16)
    pre_act = jnp.dot(normed, up_w, preferred_element_type=jnp.float32).astype(jnp.bfloat16)
    hidden = gelu_tanh(pre_act.astype(jnp.float32)).astype(jnp.bfloat16)
    return (x_f32 + jnp.dot(hidden, down_w, preferred_element_type=jnp.float32)).astype(jnp.bfloat16)


def layer_backward(layer_in, cotangent, up_w, down_w):
    x_f32 = layer_in.astype(jnp.float32)
    normed = rms_norm(x_f32).astype(jnp.bfloat16)
    pre_act = jnp.dot(normed, up_w, preferred_element_type=jnp.float32).astype(jnp.bfloat16)
    hidden = gelu_tanh(pre_act.astype(jnp.float32)).astype(jnp.bfloat16)
    grad_down = jnp.dot(hidden.T, cotangent, preferred_element_type=jnp.float32)
    d_hidden = jnp.dot(cotangent, down_w.T, preferred_element_type=jnp.float32).astype(jnp.bfloat16)
    _, gelu_back = jax.vjp(gelu_tanh, pre_act.astype(jnp.float32))
    d_pre = gelu_back(d_hidden.astype(jnp.float32))[0].astype(jnp.bfloat16)
    grad_up = jnp.dot(normed.T, d_pre, preferred_element_type=jnp.float32)
    d_normed = jnp.dot(d_pre, up_w.T, preferred_element_type=jnp.float32)
    _, norm_back = jax.vjp(rms_norm, x_f32)
    d_input = (cotangent.astype(jnp.float32) + norm_back(d_normed)[0]).astype(jnp.bfloat16)
    return d_input, grad_up, grad_down


def reference(tokens, grad_out, w_up, w_down):
    n_blocks = TOTAL_TOKENS // BLOCK_ROWS
    tok_blocks = tokens.reshape(n_blocks, BLOCK_ROWS, HIDDEN)
    grad_blocks = grad_out.reshape(n_blocks, BLOCK_ROWS, HIDDEN)

    def block_step(grad_accum, block_pair):
        accum_up, accum_down = grad_accum
        x_block, g_block = block_pair

        def fwd_step(hidden_state, weights):
            up_w, down_w = weights
            return layer_forward(hidden_state, up_w, down_w), hidden_state

        x_final, layer_inputs = lax.scan(fwd_step, x_block, (w_up, w_down))

        def bwd_step(cotangent, layer_items):
            layer_in, up_w, down_w = layer_items
            d_input, grad_up, grad_down = layer_backward(layer_in, cotangent, up_w, down_w)
            return d_input, (grad_up, grad_down)

        d_tokens, layer_grads = lax.scan(bwd_step, g_block, (layer_inputs, w_up, w_down), reverse=True)
        return (accum_up + layer_grads[0], accum_down + layer_grads[1]), (x_final, d_tokens)

    start_accum = (jnp.zeros((NUM_LAYERS, HIDDEN, FFN_DIM), jnp.float32), jnp.zeros((NUM_LAYERS, FFN_DIM, HIDDEN), jnp.float32))
    total_grads, block_outs = lax.scan(block_step, start_accum, (tok_blocks, grad_blocks))
    x_out = block_outs[0].reshape(TOTAL_TOKENS, HIDDEN)
    dx_in = block_outs[1].reshape(TOTAL_TOKENS, HIDDEN)
    return (x_out, dx_in, total_grads[0], total_grads[1])
```

```python
import functools

import jax
import jax.numpy as jnp
from jax import lax
from jax.experimental import pallas as pl
from jax.experimental.pallas import tpu as pltpu
from jax.sharding import PartitionSpec as P

NORM_EPS = 1e-6
BOTH_AXES = ('local', 'data')
CONTRACT_ROWS = (((0,), (0,)), ((), ()))
CONTRACT_COLS = (((1,), (1,)), ((), ()))
TANH_SCALE = 0.7978845608028654
TANH_CUBIC = 0.044715
STEPS = 8
PARTS = 4
N_CHUNKS = 4
VMEM_LIMIT = 62 * 1024 * 1024
F32 = jnp.float32
BF16 = jnp.bfloat16
ANY = pl.BlockSpec(memory_space=pl.ANY)


class Place:

    def __init__(self):
        self.z = lax.axis_index('local')
        self.j = lax.axis_index('data')
        self.core = lax.rem(self.j, 2)
        self.x = lax.rem(lax.div(self.j, 2), 2)
        self.y = lax.div(self.j, 4)
        self.z1 = self.z + 1 - 2 * lax.rem(self.z, 2)
        self.z2 = lax.rem(self.z + 2, 4)
        self.z3 = 3 - self.z
        self.ja = self.plane(0, 1, self.core)
        self.jb = self.plane(1, 0, self.core)
        self.jab = self.plane(1, 1, self.core)
        self.jc = self.plane(0, 0, 1 - self.core)

    def plane(self, flip_b, flip_a, core):
        y_bit = flip_b + core * (flip_a - flip_b)
        x_bit = flip_a + core * (flip_b - flip_a)
        y = self.y + y_bit - 2 * self.y * y_bit
        x = self.x + x_bit - 2 * self.x * x_bit
        return y * 4 + x * 2 + core

    def peers(self):
        return [(self.z1, self.j), (self.z2, self.j), (self.z, self.ja), (self.z, self.jb), (self.z, self.jc)]


def greet(at):
    barrier = pltpu.get_barrier_semaphore()
    for peer in at.peers():
        pl.semaphore_signal(barrier, inc=1, device_id=peer, device_id_type=pl.DeviceIdType.MESH)
    pl.semaphore_wait(barrier, 5)


def remote(src, dst, sems, k, peer):
    return pltpu.make_async_remote_copy(
        src_ref=src, dst_ref=dst, send_sem=sems[0].at[k], recv_sem=sems[1].at[k],
        device_id=peer, device_id_type=pl.DeviceIdType.MESH)


def gather_scratch(shard):
    return [
        pltpu.VMEM(shard.shape, shard.dtype),
        pltpu.SemaphoreType.DMA((2,)),
        pltpu.SemaphoreType.DMA((10,)),
        pltpu.SemaphoreType.DMA((10,)),
    ]


def gather_actions(shard, full, buf, local_sems, send_sems, recv_sems):
    at = Place()
    sems = (send_sems, recv_sems)
    j = at.j
    to_z1, to_z2 = (at.z1, j), (at.z2, j)
    to_a, to_b, to_c = (at.z, at.ja), (at.z, at.jb), (at.z, at.jc)
    columns = (j, at.ja, at.jb, at.jab)

    def load():
        return pltpu.make_async_copy(shard, buf, local_sems.at[0])

    def store():
        return pltpu.make_async_copy(buf, full.at[at.z, j], local_sems.at[1])

    def hop(k):
        src, dst, peer = (
            (lambda: shard, lambda: full.at[at.z, j], to_z2),
            (lambda: shard, lambda: full.at[at.z, j], to_z1),
            (lambda: full.at[at.z2, j], lambda: full.at[at.z2, j], to_z1),
            (lambda: full.at[:, j], lambda: full.at[:, j], to_a),
            (lambda: full.at[:, j], lambda: full.at[:, j], to_b),
            (lambda: full.at[:, at.ja], lambda: full.at[:, at.ja], to_b),
        )[k]
        return remote(src(), dst(), sems, k, peer)

    def across(k):
        return remote(full.at[:, columns[k]], full.at[:, columns[k]], sems, 6 + k, to_c)

    def first():
        greet(at)
        load().start()
        hop(0).start()
        hop(1).start()
        load().wait()
        store().start()

    def second():
        hop(0).wait_recv()
        hop(2).start()

    def third():
        store().wait()
        hop(1).wait_recv()
        hop(2).wait_recv()
        hop(4).start()
        hop(3).start()
        across(0).start()

    def fourth():
        hop(3).wait_recv()
        hop(5).start()
        across(1).start()

    def fifth():
        hop(4).wait_recv()
        across(2).start()

    def sixth():
        hop(5).wait_recv()
        across(3).start()

    def last():
        for k in range(4):
            across(k).wait_recv()
        for k in range(6):
            hop(k).wait_send()
        for k in range(4):
            across(k).wait_send()

    return [first, second, third, fourth, fifth, sixth, last]


def scatter_scratch(part):
    _, _, n, m = part.shape
    w = m // N_CHUNKS
    q = N_CHUNKS
    return [
        pltpu.VMEM((q, 2, 2, 4, n, w), F32),
        pltpu.VMEM((q, 2, 2, 4, n, w), F32),
        pltpu.VMEM((q, 2, 4, n, w), F32),
        pltpu.VMEM((q, 4, n, w), F32),
        pltpu.VMEM((q, 2, n, w), F32),
        pltpu.VMEM((q, n, w), F32),
        pltpu.SemaphoreType.DMA((q * 4,)),
        pltpu.SemaphoreType.DMA((q * 9,)),
        pltpu.SemaphoreType.DMA((q * 9,)),
    ]


def scatter_actions(part, out, own, got_core, got_b, got_a, got_z1, got_z2, local_sems, send_sems, recv_sems):
    at = Place()
    sems = (send_sems, recv_sems)
    w = out.shape[1] // N_CHUNKS
    to_z1, to_z2 = (at.z1, at.j), (at.z2, at.j)
    to_a, to_b, to_c = (at.z, at.ja), (at.z, at.jb), (at.z, at.jc)

    def load(q, b, a):
        return pltpu.make_async_copy(
            part.at[:, at.plane(b, a, at.core), :, pl.ds(q * w, w)], own.at[q, b, a], local_sems.at[q * 4 + b * 2 + a])

    def swap(q, b, a):
        return remote(part.at[:, at.plane(b, a, 1 - at.core), :, pl.ds(q * w, w)], got_core.at[q, b, a], sems, q * 9 + b * 2 + a, to_c)

    def over_b(q):
        return remote(own.at[q, 1], got_b.at[q], sems, q * 9 + 4, to_b)

    def over_a(q):
        return remote(own.at[q, 0, 1], got_a.at[q], sems, q * 9 + 5, to_a)

    def over_z1(q, k):
        return remote(own.at[q, 0, 0, (at.z1, at.z3)[k]], got_z1.at[q, k], sems, q * 9 + 6 + k, to_z1)

    def over_z2(q):
        return remote(own.at[q, 0, 0, at.z2], got_z2.at[q], sems, q * 9 + 8, to_z2)

    def begin():
        greet(at)
        for b in (1, 0):
            for q in range(N_CHUNKS):
                for a in range(2):
                    swap(q, b, a).start()
                    load(q, b, a).start()

    def chip_far(q):
        for a in range(2):
            load(q, 1, a).wait()
            swap(q, 1, a).wait_recv()
            own[q, 1, a] += got_core[q, 1, a]
        over_b(q).start()

    def chip_near(q):
        for a in range(2):
            load(q, 0, a).wait()
            swap(q, 0, a).wait_recv()
            own[q, 0, a] += got_core[q, 0, a]

    def after_b(q):
        over_b(q).wait_recv()
        own[q, 0, 1] += got_b[q, 1]
        over_a(q).start()
        own[q, 0, 0] += got_b[q, 0]

    def after_a(q):
        over_a(q).wait_recv()
        own[q, 0, 0] += got_a[q]
        for k in range(2):
            over_z1(q, k).start()

    def after_z1(q):
        for k in range(2):
            over_z1(q, k).wait_recv()
        own[q, 0, 0, at.z2] += got_z1[q, 1]
        over_z2(q).start()

    def after_z2(q):
        over_z2(q).wait_recv()
        out[:, q * w:(q + 1) * w] = own[q, 0, 0, at.z] + got_z1[q, 0] + got_z2[q]

    def end():
        for q in range(N_CHUNKS):
            for b in range(2):
                for a in range(2):
                    swap(q, b, a).wait_send()
            over_b(q).wait_send()
            over_a(q).wait_send()
            for k in range(2):
                over_z1(q, k).wait_send()
            over_z2(q).wait_send()

    return begin, chip_far, chip_near, after_b, after_a, after_z1, after_z2, end


def scatter_plan(functions, slots):
    begin, chip_far, chip_near, after_b, after_a, after_z1, after_z2, end = functions
    plan = {slot: [] for slot in range(slots)}

    def put(slot, fn):
        plan[min(slot, slots - 1)].append((slot, len(plan[min(slot, slots - 1)]), fn))

    put(0, begin)
    for q in range(N_CHUNKS):
        part = functools.partial
        put(1 + q // 2, part(chip_far, q))
        put(3, part(chip_near, q))
        put(4 + 4 * q, part(after_b, q))
        put(7 + 4 * q, part(after_a, q))
        put(9 + 4 * q, part(after_z1, q))
        put(11 + 4 * q, part(after_z2, q))
    put(10_000, end)
    return {slot: [fn for _, _, fn in sorted(entries, key=lambda e: e[:2])] for slot, entries in plan.items()}


def norm_scale(x):
    return lax.rsqrt(jnp.mean(x * x, axis=-1, keepdims=True) + NORM_EPS)


def dot(lhs, rhs):
    return jnp.dot(lhs, rhs, preferred_element_type=F32)


def dot_cols(lhs, rhs):
    return lax.dot_general(lhs, rhs, CONTRACT_COLS, preferred_element_type=F32)


def enter_pieces(x_ref, w_ref, u_ref, a_ref, s_ref):
    width = w_ref.shape[1] // PARTS

    def piece(k):
        if k == 0:
            x = x_ref[...].astype(F32)
            u_ref[...] = (x * norm_scale(x)).astype(BF16)
        cols = slice(k * width, (k + 1) * width)
        pre = dot(u_ref[...], w_ref[:, cols]).astype(BF16)
        a_ref[:, cols] = pre
        a = pre.astype(F32)
        t = jnp.tanh(a * (TANH_SCALE + (TANH_SCALE * TANH_CUBIC) * (a * a)))
        s_ref[:, cols] = (0.5 * a * (1.0 + t)).astype(BF16)

    return [functools.partial(piece, k) for k in range(PARTS)]


def leave_pieces(s_ref, x_ref, w_ref, out_ref):
    width = out_ref.shape[1] // 2

    def piece(k):
        cols = slice(k * width, (k + 1) * width)
        out_ref[:, cols] = (x_ref[:, cols].astype(F32) + dot(s_ref[...], w_ref[:, cols])).astype(BF16)

    return [functools.partial(piece, k) for k in range(2)]


def back_hidden_pieces(dy_ref, a_ref, w_ref, da_ref):
    width = a_ref.shape[1] // PARTS

    def piece(k):
        cols = slice(k * width, (k + 1) * width)
        ds = dot_cols(dy_ref[...], w_ref[cols, :]).astype(BF16).astype(F32)
        a = a_ref[:, cols].astype(F32)
        sq = a * a
        t = jnp.tanh(a * (TANH_SCALE + (TANH_SCALE * TANH_CUBIC) * sq))
        slope = (0.5 + 0.5 * t) + (a * (1.0 - t * t)) * (0.5 * TANH_SCALE + (1.5 * TANH_SCALE * TANH_CUBIC) * sq)
        da_ref[:, cols] = (ds * slope).astype(BF16)

    return [functools.partial(piece, k) for k in range(PARTS)]


def back_hidden_leave_pieces(dy_ref, a_ref, s_ref, x_ref, w_ref, da_ref, out_ref):
    return back_hidden_pieces(dy_ref, a_ref, w_ref, da_ref) + leave_pieces(s_ref, x_ref, w_ref, out_ref)


def back_input_pieces(da_ref, x_ref, dy_ref, w_ref, dx_ref, du_ref):
    width = w_ref.shape[0] // 2

    def piece(k):
        cols = slice(k * width, (k + 1) * width)
        du_ref[:, cols] = dot_cols(da_ref[...], w_ref[cols, :])
        if k == 1:
            x = x_ref[...].astype(F32)
            r = norm_scale(x)
            xr = x * r
            du = du_ref[...]
            along = jnp.mean(xr * du, axis=-1, keepdims=True)
            dx_ref[...] = (dy_ref[...].astype(F32) + r * (du - xr * along)).astype(BF16)

    return [functools.partial(piece, k) for k in range(2)]


def run_steps(pieces, plan, per_step):
    step = pl.program_id(0)
    slots_per_step = per_step
    each = len(pieces) // slots_per_step
    slots = STEPS * slots_per_step
    for part in range(slots_per_step):
        for s in range(STEPS):
            fns = plan.get(s * slots_per_step + part, []) if s * slots_per_step + part < slots else []
            if fns:
                def act(fns=fns):
                    for fn in fns:
                        fn()
                pl.when(step == s)(act)
        for piece in pieces[part * each:(part + 1) * each]:
            piece()
    rest = [fn for slot in sorted(plan) if slot >= slots for fn in plan[slot]]
    if rest:
        def finish():
            for fn in rest:
                fn()
        pl.when(step == STEPS - 1)(finish)


def row_spec(array_shape):
    return pl.BlockSpec((array_shape[0] // STEPS, array_shape[1]), lambda i: (i, 0))


def whole_spec(shape):
    return pl.BlockSpec(shape, lambda i: (0,) * len(shape), pipeline_mode=pl.Buffered(1))


def fused_call(name, make_pieces, rows_in, weight, outs, comm, comm_in, collective_id, scratch=()):
    n_in, n_out, n_scratch = len(rows_in) + 1, len(outs), len(scratch)
    per_step = 2
    out_shape = [jax.ShapeDtypeStruct(shape, dtype) for shape, dtype in outs]
    out_specs = [row_spec(shape) for shape, _ in outs]
    scratch_shapes = list(scratch)
    if comm == 'gather':
        n, m = comm_in.shape
        out_shape.append(jax.ShapeDtypeStruct((4, 8, n, m), comm_in.dtype))
        out_specs.append(ANY)
        scratch_shapes += gather_scratch(comm_in)
    else:
        _, _, n, m = comm_in.shape
        out_shape.append(jax.ShapeDtypeStruct((n, m), F32))
        out_specs.append(pl.BlockSpec((n, m), lambda i: (0, 0)))
        scratch_shapes += scatter_scratch(comm_in)

    def kernel(*refs):
        ins, comm_ref = refs[:n_in], refs[n_in]
        out_refs, comm_out = refs[n_in + 1:n_in + 1 + n_out], refs[n_in + 1 + n_out]
        rest = refs[n_in + 2 + n_out:]
        own, comm_scratch = rest[:n_scratch], rest[n_scratch:]
        if comm == 'gather':
            acts = gather_actions(comm_ref, comm_out, *comm_scratch)
            slots = (0, 2, 4, 8, 9, 13, 10_000)
            plan = {slot: [fn] for slot, fn in zip(slots, acts)}
        else:
            functions = scatter_actions(comm_ref, comm_out, *comm_scratch)
            plan = scatter_plan(functions, STEPS * per_step + 1)
        run_steps(make_pieces(*ins, *out_refs, *own), plan, per_step)

    rows = rows_in[0].shape[0]
    flops = 2 * rows * weight.size
    result = pl.pallas_call(
        kernel,
        grid=(STEPS,),
        out_shape=out_shape,
        in_specs=[row_spec(v.shape) for v in rows_in] + [whole_spec(weight.shape), ANY],
        out_specs=out_specs,
        scratch_shapes=scratch_shapes,
        compiler_params=pltpu.CompilerParams(
            dimension_semantics=('arbitrary',), collective_id=collective_id, has_side_effects=True, vmem_limit_bytes=VMEM_LIMIT),
        cost_estimate=pl.CostEstimate(flops=2 * flops, bytes_accessed=64 << 20, transcendentals=0),
        name=name,
    )(*rows_in, weight, comm_in)
    if comm == 'gather':
        result = [*result[:-1], result[-1].reshape(32 * comm_in.shape[0], comm_in.shape[1])]
    return result


def gather_alone(shard, collective_id):
    n, m = shard.shape

    def kernel(shard_ref, full_ref, *scratch):
        for fn in gather_actions(shard_ref, full_ref, *scratch):
            fn()

    full = pl.pallas_call(
        kernel,
        out_shape=jax.ShapeDtypeStruct((4, 8, n, m), shard.dtype),
        in_specs=[ANY],
        out_specs=ANY,
        scratch_shapes=gather_scratch(shard),
        compiler_params=pltpu.CompilerParams(collective_id=collective_id, has_side_effects=True, vmem_limit_bytes=VMEM_LIMIT),
        cost_estimate=pl.CostEstimate(flops=1 << 34, bytes_accessed=16 << 20, transcendentals=0),
        name='gather_alone',
    )(shard)
    return full.reshape(32 * n, m)


def solution(mesh):
    tok_spec = P(BOTH_AXES, None)
    w_spec = P(None, BOTH_AXES, None)

    def device_fn(tokens, grad_out, w_up, w_down):
        t, d = tokens.shape
        f = w_up.shape[2]
        wide, narrow = ((t, f), BF16), ((t, d), BF16)

        def again(shard, value):
            shard, _ = lax.optimization_barrier((shard, value))
            return lax.all_gather(shard, BOTH_AXES, axis=0, tiled=True)

        def grad(lhs, rhs):
            part = lax.dot_general(lhs, rhs, CONTRACT_ROWS, preferred_element_type=F32)
            return part.reshape(4, 8, part.shape[0] // 32, part.shape[1])

        up0 = gather_alone(w_up[0], 0)
        u0, a0, s0, down0 = fused_call('enter_0', enter_pieces, [tokens], up0, [narrow, wide, wide], 'gather', w_down[0], 1)
        mid, up1 = fused_call('leave_0', leave_pieces, [s0, tokens], down0, [narrow], 'gather', w_up[1], 2)
        u1, a1, s1, down1 = fused_call('enter_1', enter_pieces, [mid], up1, [narrow, wide, wide], 'gather', w_down[1], 3)
        up1_again = again(w_up[1], s1)
        part = grad(s1, grad_out)
        da1, x_out, grad_down1 = fused_call(
            'back_hidden_1', back_hidden_leave_pieces, [grad_out, a1, s1, mid], down1, [wide, narrow], 'scatter', part, 4)
        down0_again = again(w_down[0], da1)
        up0_again = again(w_up[0], da1)
        part = grad(u1, da1)
        du_scratch = [pltpu.VMEM((t // STEPS, d), F32)]
        d_mid, grad_up1 = fused_call('back_input_1', back_input_pieces, [da1, mid, grad_out], up1_again, [narrow], 'scatter', part, 5, du_scratch)
        part = grad(s0, d_mid)
        da0, grad_down0 = fused_call('back_hidden_0', back_hidden_pieces, [d_mid, a0], down0_again, [wide], 'scatter', part, 6)
        part = grad(u0, da0)
        dx_in, grad_up0 = fused_call('back_input_0', back_input_pieces, [da0, tokens, d_mid], up0_again, [narrow], 'scatter', part, 7, du_scratch)
        return x_out, dx_in, jnp.stack([grad_up0, grad_up1]), jnp.stack([grad_down0, grad_down1])

    return jax.shard_map(device_fn, mesh=mesh, in_specs=(tok_spec, tok_spec, w_spec, w_spec), out_specs=(tok_spec, tok_spec, w_spec, w_spec), check_vma=False)
```
